128 devices in a mesh: groups: 4 (over x, y), lon: 16 (over z), lat: 2 (over core).
Axes of the slice: x: 2, y: 2, z: 16, core: 2. Of those that a mesh axis runs over, the one named last changes fastest.
The devices are a block of a 8x8x16 slice.
Arguments:
- fields: bfloat16 [48, 2048, 128], P(('groups', 'lat'), 'lon'), parts along dimension 0, may hold values from -6 to 6
- norm_gain: float32 [128], replicated, may hold values from 0.5 to 1.5
- w_qkv: bfloat16 [128, 384], replicated, may hold values from -5.303301 to 5.303301
- w_out: bfloat16 [128, 128], replicated, may hold values from -0.5 to 0.5
Outputs:
- updated: bfloat16 [48, 2048, 128], P(('groups', 'lat'), 'lon'), parts along dimension 0
The draws below stay inside these ranges and needn't reach their ends.
There are 4 independent parts, one for each index of `groups`. The reference program is written for one: setup_inputs(seed, part) draws one part's arguments, and reference() takes and returns one part's arrays. A program takes and returns all parts, laid end to end along the dimension named above; an argument that names none is the same for every part. Nothing has to cross between parts.
All inputs are finite; a program needn't handle non-finite values.
Results may differ from the reference program's by a relative error of at most 0.005.
The reference program's roundings to bfloat16 on the way (of `normed`, `weights` and `attended`) count: a program that leaves them out, or rounds other values in their place, can miss the bound.
Values may be sent and summed in bfloat16 or wider, within the bound.
A program may use at most 128 MiB of HBM per device.

```python
import math
import jax
import jax.numpy as jnp
from jax import lax

HEADS = 8
HEAD_DIM = 16
C = 128
NLON = 2048
NLAT = 12


def draw_w_qkv(key, part):
    base = jnp.clip(jax.random.normal(key, (C, 3 * C), jnp.float32), -6.0, 6.0) * (2.0 / math.sqrt(C))
    return base.astype(jnp.bfloat16)


def block_scale(stream_key, shape, shards, low, high):
    def one(position, shards_of):
        steps = jax.random.uniform(jax.random.fold_in(jax.random.fold_in(stream_key, 6), position), (shards_of,), jnp.float32, low / len(shards), high / len(shards))
        return jnp.repeat(jnp.exp(steps), shape[position] // shards_of).reshape((-1,) + (1,) * (len(shape) - position - 1))

    loudness = one(*shards[0])
    for cut in shards[1:]:
        loudness = loudness * one(*cut)
    return loudness


def bell_draw(rng, dims, scale, bound, split=(), kind=jnp.bfloat16):
    values = scale * jax.random.normal(rng, dims, jnp.float32)
    if split:
        values = values * block_scale(rng, dims, split, -0.22, 0.18)
    return jnp.clip(values, -bound, bound).astype(kind)


def setup_inputs(seed: int = 0, part: int = 0) -> dict:
    key_list = jax.random.split(jax.random.key(seed), 5)
    part_keys = jax.random.split(jax.random.fold_in(key_list[4], part), 5)
    fields = bell_draw(part_keys[0], (NLAT, NLON, C), 1.0, 6.0, ((0, 2), (1, 16)))
    norm_gain = jnp.clip(1.0 + 0.1 * jax.random.normal(key_list[1], (C,), jnp.float32), 0.5, 1.5)
    w_qkv = draw_w_qkv(jax.random.fold_in(key_list[4], 71), part)
    w_out = bell_draw(key_list[3], (C, C), C ** -0.5, 0.5)
    return {"fields": fields, "norm_gain": norm_gain, "w_qkv": w_qkv, "w_out": w_out}


def reference(fields, norm_gain, w_qkv, w_out):
    width = HEADS * HEAD_DIM
    inputs = fields.astype(jnp.float32)
    center = lax.optimization_barrier(jnp.mean(inputs, axis=-1, keepdims=True))
    spread = lax.optimization_barrier(jnp.mean((inputs - center) ** 2, axis=-1, keepdims=True))
    normed = ((inputs - center) * lax.rsqrt(spread + 1e-05) * norm_gain).astype(jnp.bfloat16)
    projected = jnp.dot(normed.reshape(-1, width), w_qkv, preferred_element_type=jnp.float32)
    projected = projected.reshape(NLAT, NLON, 3 * width)
    queries = (projected[..., :width] * (1.0 / math.sqrt(HEAD_DIM))).astype(jnp.bfloat16)
    keys = projected[..., width:2 * width].astype(jnp.bfloat16)
    values = projected[..., 2 * width:].astype(jnp.bfloat16)
    block = math.gcd(NLON, 512)

    def one_row(operands):
        row_queries, row_keys, row_values = operands
        key_heads = row_keys.reshape(NLON, HEADS, HEAD_DIM).astype(jnp.float32)
        value_heads = row_values.reshape(NLON, HEADS, HEAD_DIM).astype(jnp.float32)
        query_blocks = row_queries.reshape(NLON // block, block, HEADS, HEAD_DIM)

        def one_block(query_block):
            scores = jnp.einsum('qhd,khd->hqk', query_block.astype(jnp.float32), key_heads)
            highest = lax.optimization_barrier(jnp.max(scores, axis=-1, keepdims=True))
            expd = jnp.exp(scores - highest)
            totals = lax.optimization_barrier(jnp.sum(expd, axis=-1))
            weights = expd.astype(jnp.bfloat16).astype(jnp.float32)
            mixed = jnp.einsum('hqk,khd->qhd', weights, value_heads)
            mixed = mixed / jnp.transpose(totals)[:, :, None]
            return mixed.reshape(block, width).astype(jnp.bfloat16)
        return lax.map(one_block, query_blocks).reshape(NLON, width)
    attended = lax.map(one_row, (queries, keys, values))
    output = jnp.dot(attended.reshape(-1, width), w_out, preferred_element_type=jnp.float32)
    return (inputs + output.reshape(NLAT, NLON, width)).astype(jnp.bfloat16)
```

```python
import functools
import math

import jax
import jax.numpy as jnp
from jax import lax
from jax.experimental import pallas as pl
from jax.experimental.pallas import tpu as pltpu
from jax.sharding import PartitionSpec as P

HEADS = 8
LOG2E = math.log2(math.e)
LOW = -1e30
F32 = jnp.float32
BF16 = jnp.bfloat16
MESH = pl.DeviceIdType.MESH


def kernel(
    n,
    fields_ref, gain_ref, wqkv_ref, wout_ref, out_ref,
    xin, gain, wqkv, wout, raw, nbuf, kd, vt, qt, qh, sbuf, mst, ost, alpha, att, obuf,
    load_sem, raw_send, raw_recv, fwd_send, out_send, out_recv, ready,
):
    rows, cells, width = xin.shape
    total_rows = 2 * rows
    half = cells // 2
    hw = width // HEADS
    span = 4 * cells
    keys = 8 * cells
    tiles = 4
    tile = keys // tiles

    p = lax.axis_index("lon")
    j = lax.axis_index("lat")
    right = {"lon": lax.rem(p + 1, n), "lat": j}
    left = {"lon": lax.rem(p + n - 1, n), "lat": j}
    partner = {"lon": p, "lat": 1 - j}

    loads = [
        pltpu.make_async_copy(fields_ref, xin, load_sem.at[0]),
        pltpu.make_async_copy(gain_ref, gain, load_sem.at[1]),
        pltpu.make_async_copy(wqkv_ref, wqkv, load_sem.at[2]),
        pltpu.make_async_copy(wout_ref, wout, load_sem.at[3]),
    ]
    for load in loads:
        load.start()

    barrier = pltpu.get_barrier_semaphore()
    for step in (1, n - 1):
        for core in (0, 1):
            pl.semaphore_signal(
                barrier, inc=1, device_id={"lon": lax.rem(p + step, n), "lat": core}, device_id_type=MESH
            )
    pl.semaphore_signal(barrier, inc=1, device_id=partner, device_id_type=MESH)

    def row_of(x):
        return (x * total_rows + n - 1) // n

    def takes_row(x):
        return (row_of(x) * n) // total_rows == x

    my_row = row_of(p)
    main = takes_row(p)
    my_lat = my_row // rows
    my_r = lax.rem(my_row, rows)

    def field_copy(d, h):
        x = lax.rem(p + n - d, n)
        r = lax.rem(row_of(x), rows)
        return pltpu.make_async_remote_copy(
            src_ref=xin.at[r, pl.ds(h * half, half)],
            dst_ref=raw.at[d, pl.ds(h * half, half)],
            send_sem=raw_send.at[d, h],
            recv_sem=raw_recv.at[d, h],
            device_id={"lon": x, "lat": h},
            device_id_type=MESH,
        )

    def own_field_copy(h):
        return pltpu.make_async_copy(
            fields_ref.at[my_r, pl.ds(h * half, half)], raw.at[0, pl.ds(h * half, half)], raw_recv.at[0, h]
        )

    def sends_to(d):
        x = lax.rem(p + n - d, n)
        return jnp.logical_and(takes_row(x), row_of(x) // rows == j)

    def start_fields(d):
        @pl.when(sends_to(d))
        def _():
            for h in (0, 1):
                if d == 0:
                    @pl.when(j == h)
                    def _():
                        own_field_copy(h).start()

                    @pl.when(j != h)
                    def _():
                        field_copy(d, h).start()
                else:
                    field_copy(d, h).start()

    def forward(d):
        return pltpu.make_async_remote_copy(
            src_ref=raw.at[d, pl.ds(j * half, half)],
            dst_ref=raw.at[d, pl.ds(j * half, half)],
            send_sem=fwd_send.at[d],
            recv_sem=raw_recv.at[d, j],
            device_id=partner,
            device_id_type=MESH,
        )

    def wait_half(d, h):
        pltpu.make_async_copy(
            fields_ref.at[0, pl.ds(0, half)], raw.at[d, pl.ds(h * half, half)], raw_recv.at[d, h]
        ).wait()

    def take(d):
        wait_half(d, j)
        forward(d).start()

    loads[0].wait()
    pl.semaphore_wait(barrier, 5)
    start_fields(0)
    for dist in range(1, n // 2 + 1):
        if dist > 1:
            for side in (right, left):
                pl.semaphore_signal(ready.at[dist - 2], inc=1, device_id=side, device_id_type=MESH)
            pl.semaphore_wait(ready.at[dist - 2], 2)
        start_fields(dist)
        if dist < n // 2:
            start_fields(n - dist)

    for load in loads[1:]:
        load.wait()

    def out_copy(g, k):
        d = own_chunk(g, k)
        return pltpu.make_async_remote_copy(
            src_ref=obuf.at[g, pl.ds(k * cells, cells)],
            dst_ref=out_ref.at[my_r],
            send_sem=out_send.at[g, k],
            recv_sem=out_recv.at[my_r],
            device_id={"lon": lax.rem(p + d, n), "lat": my_lat},
            device_id_type=MESH,
        )

    def own_out_copy():
        return pltpu.make_async_copy(obuf.at[0, pl.ds(0, cells)], out_ref.at[my_r], out_recv.at[my_r])

    def own_chunk(g, k):
        return 4 * g + k + j * (n - 1 - 8 * g - 2 * k)

    @pl.when(main)
    def _():
        wq = wqkv[:, :width]
        wk = wqkv[:, width : 2 * width]
        wv = wqkv[:, 2 * width :]
        for h in range(HEADS):
            vt[pl.ds(2 * hw * h + hw, hw), :] = jnp.ones((hw, n * cells), BF16)
        qh[...] = jnp.zeros_like(qh)
        mst[...] = jnp.full(mst.shape, LOW, F32)
        ost[...] = jnp.zeros_like(ost)

        def project(slot, d, place):
            x = raw[d].astype(F32)
            center = jnp.mean(x, axis=-1, keepdims=True)
            y = x - center
            spread = jnp.mean(y * y, axis=-1, keepdims=True)
            normed = (y * lax.rsqrt(spread + 1e-05) * gain[...]).astype(BF16)
            nbuf[place] = normed
            where = pl.ds(pl.multiple_of(slot * cells, cells), cells)
            k = jnp.dot(normed, wk, preferred_element_type=F32).astype(BF16)
            kd[where, :width] = k
            kd[where, width:] = k
            v = lax.dot_general(wv, normed, (((0,), (1,)), ((), ())), preferred_element_type=F32).astype(BF16)
            for h in range(HEADS):
                vt[2 * hw * h : 2 * hw * h + hw, where] = v[hw * h : hw * h + hw]

        def arrive(g):
            def first(k, carry):
                take(4 * g + k)
                take(n - 1 - 4 * g - k)
                return carry

            lax.fori_loop(0, 4, first, 0)

            def second(k, carry):
                for place in (0, 1):
                    d = 4 * g + k if place == 0 else n - 1 - 4 * g - k
                    wait_half(d, 1 - j)
                    project(8 * g + 4 * place + k, d, place)
                q = lax.dot_general(wq, nbuf[j], (((0,), (1,)), ((), ())), preferred_element_type=F32)
                q = (q * (1.0 / math.sqrt(hw))).astype(BF16).astype(F32) * LOG2E
                high = q.astype(BF16)
                low = (q - high.astype(F32)).astype(BF16)
                where = pl.ds(pl.multiple_of(k * cells, cells), cells)
                qt[g, :width, where] = high
                qt[g, width:, where] = low
                return carry

            lax.fori_loop(0, 4, second, 0)

        def scores(h, g, kb, slot):
            before = lax.rem(h + HEADS - 1, HEADS)
            for base in (0, width):
                qh[pl.ds(base + pl.multiple_of(before * hw, hw), hw), :] = jnp.zeros((hw, span), BF16)
            for base in (0, width):
                here = pl.ds(base + pl.multiple_of(h * hw, hw), hw)
                qh[here, :] = qt[g, here, :]
            high = None
            for t in range(tiles):
                s = jnp.dot(
                    kd[pl.ds(pl.multiple_of(kb * keys, keys) + t * tile, tile), :], qh[...], preferred_element_type=F32
                )
                sbuf[slot, pl.ds(t * tile, tile), :] = s
                top = jnp.max(s.reshape(tile // 8, 8, span), axis=0)
                high = top if high is None else jnp.maximum(high, top)
            old = mst[g, h]
            new = jnp.maximum(old, jnp.max(high, axis=0, keepdims=True))
            mst[g, h] = new
            alpha[slot, 0] = new
            alpha[slot, 1] = jnp.exp2(old - new)

        def values(h, g, kb, slot):
            top = alpha[slot, 0]
            total = ost[g, h] * alpha[slot, 1]
            for t in range(tiles):
                e = jnp.exp2(sbuf[slot, pl.ds(t * tile, tile), :] - top).astype(BF16)
                v = vt[
                    pl.ds(pl.multiple_of(2 * hw * h, 2 * hw), 2 * hw),
                    pl.ds(pl.multiple_of(kb * keys, keys) + t * tile, tile),
                ]
                total = total + jnp.dot(v, e, preferred_element_type=F32)
            ost[g, h] = total
            att[pl.ds(pl.multiple_of(h * hw, hw), hw), :] = (total[:hw] / total[hw:]).astype(BF16)

        def run(units):
            for g, kb in units:
                scores(0, g, kb, 0)

                def step(h, carry):
                    scores(h + 1, g, kb, lax.rem(h + 1, 2))
                    values(h, g, kb, lax.rem(h, 2))
                    return carry

                lax.fori_loop(0, HEADS - 1, step, 0)
                values(HEADS - 1, g, kb, (HEADS - 1) % 2)

        def finish(g):
            result = lax.dot_general(
                att[...], wout[...], (((0,), (0,)), ((), ())), preferred_element_type=F32
            )
            for k in range(4):
                d = own_chunk(g, k)
                here = pl.ds(k * cells, cells)
                obuf[g, here, :] = (result[k * cells : (k + 1) * cells] + raw[d].astype(F32)).astype(BF16)
            for k in (3, 2, 1, 0):
                if g == 0 and k == 0:
                    own = jnp.logical_and(j == 0, my_lat == 0)

                    @pl.when(own)
                    def _():
                        own_out_copy().start()

                    @pl.when(jnp.logical_not(own))
                    def _():
                        out_copy(g, k).start()
                else:
                    out_copy(g, k).start()

        arrive(0)
        run([(0, 0)])
        arrive(1)
        run([(1, 0), (1, 1)])
        finish(1)
        run([(0, 1)])
        finish(0)

    for d in range(n):
        @pl.when(sends_to(d))
        def _():
            for h in (0, 1):
                if d == 0:
                    @pl.when(j != h)
                    def _():
                        field_copy(d, h).wait_send()
                else:
                    field_copy(d, h).wait_send()

    @pl.when(main)
    def _():
        for d in range(n):
            forward(d).wait_send()
        for g in (0, 1):
            for k in range(4):
                if g == 0 and k == 0:
                    @pl.when(jnp.logical_not(jnp.logical_and(j == 0, my_lat == 0)))
                    def _():
                        out_copy(g, k).wait_send()
                else:
                    out_copy(g, k).wait_send()

    for r in range(rows):
        pltpu.make_async_copy(fields_ref.at[0], out_ref.at[r], out_recv.at[r]).wait()


def body(n, fields, norm_gain, w_qkv, w_out):
    rows, cells, width = fields.shape
    hw = width // HEADS
    span, keys = 4 * cells, 8 * cells
    hbm = pl.BlockSpec(memory_space=pl.ANY)
    scratch = [
        pltpu.VMEM((rows, cells, width), BF16),
        pltpu.VMEM((1, width), F32),
        pltpu.VMEM((width, 3 * width), BF16),
        pltpu.VMEM((width, width), BF16),
        pltpu.VMEM((n, cells, width), BF16),
        pltpu.VMEM((2, cells, width), BF16),
        pltpu.VMEM((n * cells, 2 * width), BF16),
        pltpu.VMEM((2 * width, n * cells), BF16),
        pltpu.VMEM((2, 2 * width, span), BF16),
        pltpu.VMEM((2 * width, span), BF16),
        pltpu.VMEM((2, keys, span), F32),
        pltpu.VMEM((2, HEADS, 1, span), F32),
        pltpu.VMEM((2, HEADS, 2 * hw, span), F32),
        pltpu.VMEM((2, 2, 1, span), F32),
        pltpu.VMEM((width, span), BF16),
        pltpu.VMEM((2, span, width), BF16),
        pltpu.SemaphoreType.DMA((4,)),
        pltpu.SemaphoreType.DMA((n, 2)),
        pltpu.SemaphoreType.DMA((n, 2)),
        pltpu.SemaphoreType.DMA((n,)),
        pltpu.SemaphoreType.DMA((2, 4)),
        pltpu.SemaphoreType.DMA((rows,)),
        pltpu.SemaphoreType.REGULAR((n // 2 - 1,)),
    ]
    return pl.pallas_call(
        functools.partial(kernel, n),
        out_shape=jax.ShapeDtypeStruct(fields.shape, fields.dtype),
        in_specs=[hbm] * 4,
        out_specs=hbm,
        scratch_shapes=scratch,
        compiler_params=pltpu.CompilerParams(collective_id=0, has_side_effects=True),
        name="axial",
    )(fields, norm_gain.reshape(1, width), w_qkv, w_out)


def solution(mesh):
    return jax.shard_map(
        functools.partial(body, mesh.shape["lon"]),
        mesh=mesh,
        in_specs=(P(("groups", "lat"), "lon", None), P(), P(), P()),
        out_specs=P(("groups", "lat"), "lon", None),
        check_vma=False,
    )
```

```python
import functools
import math

import jax
import jax.numpy as jnp
from jax import lax
from jax.experimental import pallas as pl
from jax.experimental.pallas import tpu as pltpu
from jax.sharding import PartitionSpec as P

HEADS = 8
LOG2E = math.log2(math.e)
LOW = -1e30
AHEAD = 2
PLAN = [[], [(1, 0), (1, 1)], [(2, 0), (2, 1), (2, 2)], [(2, 3), (3, 0), (3, 1), (3, 2), (3, 3), (1, 2), (1, 3), (0, 0), (0, 1), (0, 2), (0, 3)]]
F32 = jnp.float32
BF16 = jnp.bfloat16
MESH = pl.DeviceIdType.MESH


def kernel(
    n,
    fields_ref, gain_ref, wqkv_ref, wout_ref, out_ref,
    xin, gain, wqkv, wout, raw, nbuf, kd, vt, qt, sbuf0, sbuf1, sbuf2, sbuf3, mst, ost, alpha, att, obuf,
    load_sem, raw_send, raw_recv, fwd_send, out_send, out_recv, ready,
):
    rows, cells, width = xin.shape
    total_rows = 2 * rows
    half = cells // 2
    hw = width // HEADS
    span = 2 * cells
    tile = 2 * cells
    keys = 4 * cells
    sbufs = (sbuf0, sbuf1, sbuf2, sbuf3)

    p = lax.axis_index("lon")
    j = lax.axis_index("lat")
    right = {"lon": lax.rem(p + 1, n), "lat": j}
    left = {"lon": lax.rem(p + n - 1, n), "lat": j}
    partner = {"lon": p, "lat": 1 - j}

    loads = [
        pltpu.make_async_copy(fields_ref, xin, load_sem.at[0]),
        pltpu.make_async_copy(gain_ref, gain, load_sem.at[1]),
        pltpu.make_async_copy(wqkv_ref, wqkv, load_sem.at[2]),
        pltpu.make_async_copy(wout_ref, wout, load_sem.at[3]),
    ]
    for load in loads:
        load.start()

    barrier = pltpu.get_barrier_semaphore()
    for dist in range(n // 4, 0, -1):
        for step in {dist, n - dist}:
            for core in (0, 1):
                pl.semaphore_signal(
                    barrier, inc=1, device_id={"lon": lax.rem(p + step, n), "lat": core}, device_id_type=MESH
                )
    pl.semaphore_signal(barrier, inc=1, device_id=partner, device_id_type=MESH)

    def row_of(x):
        return (x * total_rows + n - 1) // n

    def takes_row(x):
        return (row_of(x) * n) // total_rows == x

    my_row = row_of(p)
    main = takes_row(p)
    my_lat = my_row // rows
    my_r = lax.rem(my_row, rows)

    def field_copy(d, h):
        x = lax.rem(p + n - d, n)
        r = lax.rem(row_of(x), rows)
        return pltpu.make_async_remote_copy(
            src_ref=xin.at[r, pl.ds(h * half, half)],
            dst_ref=raw.at[d, pl.ds(h * half, half)],
            send_sem=raw_send.at[d, h],
            recv_sem=raw_recv.at[d, h],
            device_id={"lon": x, "lat": h},
            device_id_type=MESH,
        )

    def own_field_copy(h):
        return pltpu.make_async_copy(
            fields_ref.at[my_r, pl.ds(h * half, half)], raw.at[0, pl.ds(h * half, half)], raw_recv.at[0, h]
        )

    def sends_to(d):
        x = lax.rem(p + n - d, n)
        return jnp.logical_and(takes_row(x), row_of(x) // rows == j)

    def start_fields(d):
        @pl.when(sends_to(d))
        def _():
            for h in (0, 1):
                if d == 0:
                    @pl.when(j == h)
                    def _():
                        own_field_copy(h).start()

                    @pl.when(j != h)
                    def _():
                        field_copy(d, h).start()
                else:
                    field_copy(d, h).start()

    def forward(d):
        return pltpu.make_async_remote_copy(
            src_ref=raw.at[d, pl.ds(j * half, half)],
            dst_ref=raw.at[d, pl.ds(j * half, half)],
            send_sem=fwd_send.at[d],
            recv_sem=raw_recv.at[d, j],
            device_id=partner,
            device_id_type=MESH,
        )

    def wait_half(d, h):
        pltpu.make_async_copy(
            fields_ref.at[0, pl.ds(0, half)], raw.at[d, pl.ds(h * half, half)], raw_recv.at[d, h]
        ).wait()

    def take(d):
        wait_half(d, j)
        forward(d).start()

    loads[0].wait()
    pl.semaphore_wait(barrier, n + 1)
    for step in (n // 4, n - n // 4):
        pl.semaphore_signal(
            ready.at[0], inc=1, device_id={"lon": lax.rem(p + step, n), "lat": j}, device_id_type=MESH
        )
    start_fields(0)
    for dist in range(1, n // 4 + 1):
        start_fields(dist)
        start_fields(n - dist)
    pl.semaphore_wait(ready.at[0], 2)
    for dist in range(n // 2, n // 4, -1):
        start_fields(dist)
        if dist < n // 2:
            start_fields(n - dist)

    for load in loads[1:]:
        load.wait()

    def stage_chunks(g):
        return (2 * g, 2 * g + 1), (n - 1 - 2 * g, n - 2 - 2 * g)

    def own_chunk(g, k):
        return 2 * g + k + j * (n - 1 - 4 * g - 2 * k)

    def order_of(s):
        return s + s // 2 - 2 * (s // 3)

    def out_copy(s, k):
        d = own_chunk(order_of(s), k)
        return pltpu.make_async_remote_copy(
            src_ref=obuf.at[s, pl.ds(k * cells, cells)],
            dst_ref=out_ref.at[my_r],
            send_sem=out_send.at[s, k],
            recv_sem=out_recv.at[my_r],
            device_id={"lon": lax.rem(p + d, n), "lat": my_lat},
            device_id_type=MESH,
        )

    own_out = jnp.logical_and(j == 0, my_lat == 0)

    def own_out_copy():
        return pltpu.make_async_copy(obuf.at[0, pl.ds(0, cells)], out_ref.at[my_r], out_recv.at[my_r])

    @pl.when(main)
    def _():
        wq = wqkv[:, :width]
        wk = wqkv[:, width : 2 * width]
        wv = wqkv[:, 2 * width :]
        for h in range(HEADS):
            vt[pl.ds(2 * hw * h + hw, hw), :] = jnp.ones((hw, n * cells), BF16)

        def clear(h, carry):
            for s in range(4):
                mst[s, h] = jnp.full(mst.shape[2:], LOW, F32)
                ost[s, h] = jnp.zeros(ost.shape[2:], F32)
            return carry

        lax.fori_loop(0, HEADS, clear, 0)

        def project(slot, d, place):
            x = raw[d].astype(F32)
            center = jnp.mean(x, axis=-1, keepdims=True)
            y = x - center
            spread = jnp.mean(y * y, axis=-1, keepdims=True)
            normed = (y * lax.rsqrt(spread + 1e-05) * gain[...]).astype(BF16)
            nbuf[place] = normed
            where = pl.ds(slot * cells, cells)
            k = jnp.dot(normed, wk, preferred_element_type=F32).astype(BF16)
            kd[where, :width] = k
            kd[where, width:] = k
            v = lax.dot_general(wv, normed, (((0,), (1,)), ((), ())), preferred_element_type=F32).astype(BF16)
            for h in range(HEADS):
                vt[2 * hw * h : 2 * hw * h + hw, where] = v[hw * h : hw * h + hw]

        def arrive(s):
            sides = stage_chunks(order_of(s))
            for k in (0, 1):
                for side in sides:
                    take(side[k])
            for k in (0, 1):
                for place in (0, 1):
                    d = sides[place][k]
                    wait_half(d, 1 - j)
                    project(4 * s + 2 * place + k, d, place)
                q = lax.dot_general(wq, nbuf[j], (((0,), (1,)), ((), ())), preferred_element_type=F32)
                q = (q * (1.0 / math.sqrt(hw))).astype(BF16).astype(F32) * LOG2E
                high = q.astype(BF16)
                low = (q - high.astype(F32)).astype(BF16)
                where = pl.ds(k * cells, cells)
                qt[s, :width, where] = high
                qt[s, width:, where] = low

        def score_steps(unit, slot):
            heads, qb, kg = unit
            high = {}

            def queries(h):
                gap = jnp.zeros((hw, span), BF16)
                return jnp.concatenate(
                    [
                        qt[qb, pl.ds(base + hw * other, hw), :] if other == h else gap
                        for base in (0, width)
                        for other in range(HEADS)
                    ],
                    axis=0,
                )

            of = [queries(h) for h in heads]

            def step(t):
                for i, q in enumerate(of):
                    where = pl.ds(pl.multiple_of(kg * keys, keys) + t * tile, tile)
                    s = jnp.dot(kd[where, :], q, preferred_element_type=F32)
                    sbufs[slot][i, pl.ds(t * tile, tile), :] = s
                    peak = jnp.max(s.reshape(tile // 8, 8, span), axis=0)
                    high[i] = peak if t == 0 else jnp.maximum(high[i], peak)

            def end():
                for i, h in enumerate(heads):
                    old = mst[qb, h]
                    new = jnp.maximum(old, jnp.max(high[i], axis=0, keepdims=True))
                    mst[qb, h] = new
                    alpha[slot, i, 0] = new
                    alpha[slot, i, 1] = jnp.exp2(old - new)

            return step, end

        def value_steps(unit, slot):
            heads, qb, kg = unit
            total = {i: ost[qb, h] * alpha[slot, i, 1] for i, h in enumerate(heads)}

            def step(t):
                for i, h in enumerate(heads):
                    e = jnp.exp2(sbufs[slot][i, pl.ds(t * tile, tile), :] - alpha[slot, i, 0]).astype(BF16)
                    where = pl.ds(pl.multiple_of(kg * keys, keys) + t * tile, tile)
                    v = vt[pl.ds(2 * hw * h, 2 * hw), where]
                    total[i] = total[i] + jnp.dot(v, e, preferred_element_type=F32)

            def end():
                for i, h in enumerate(heads):
                    ost[qb, h] = total[i]
                    att[qb, pl.ds(h * hw, hw), :] = (total[i][:hw] / total[i][hw:]).astype(BF16)

            return step, end

        def both(score_of, value_of):
            a = None if score_of is None else score_steps(*score_of)
            b = None if value_of is None else value_steps(*value_of)
            for t in range(keys // tile):
                if a:
                    a[0](t)
                if b:
                    b[0](t)
            if a:
                a[1]()
            if b:
                b[1]()

        units = HEADS // 2

        def run(combo, count, final):
            def unit(i, a):
                qb, kg = combo(i + a // units)
                a = a % units
                return ((2 * a, 2 * a + 1), qb, kg), a

            for a in range(AHEAD):
                both(unit(0, a), None)

            def step(i, carry):
                for a in range(units):
                    both(unit(i, a + AHEAD), unit(i, a))
                if final:
                    qb, kg = combo(i)

                    @pl.when(kg == 3)
                    def _():
                        finish(qb)

                return carry

            if count > 1:
                lax.fori_loop(0, count - 1, step, 0)
            for a in range(units):
                both(unit(count - 1, a + AHEAD) if a + AHEAD < units else None, unit(count - 1, a))
            if final:
                finish(combo(count - 1)[0])

        def finish(s):
            result = lax.dot_general(
                att[s], wout[...], (((0,), (0,)), ((), ())), preferred_element_type=F32
            )
            group = order_of(s)
            for k in (1, 0):
                here = pl.ds(k * cells, cells)
                d = own_chunk(group, k)
                obuf[s, here, :] = (result[k * cells : (k + 1) * cells] + raw[d].astype(F32)).astype(BF16)
                if k == 0:
                    own = jnp.logical_and(own_out, s == 0)

                    @pl.when(own)
                    def _():
                        own_out_copy().start()

                    @pl.when(jnp.logical_not(own))
                    def _():
                        out_copy(s, k).start()
                else:
                    out_copy(s, k).start()

        def pick(values, i):
            count = len(values)
            got = values[0]
            for k in range(1, count):
                if values[k] != values[k - 1]:
                    got = got + (values[k] - values[k - 1]) * ((i + count - k) // count)
            return got

        for s, combos in enumerate(PLAN):
            arrive(s)
            if combos:
                blocks, groups = zip(*combos)
                run(lambda i, b=blocks, g=groups: (pick(b, i), pick(g, i)), len(combos), s == 3)

    for d in range(n):
        @pl.when(sends_to(d))
        def _():
            for h in (0, 1):
                if d == 0:
                    @pl.when(j != h)
                    def _():
                        field_copy(d, h).wait_send()
                else:
                    field_copy(d, h).wait_send()

    @pl.when(main)
    def _():
        for d in range(n):
            forward(d).wait_send()
        for s in range(4):
            for k in (0, 1):
                if s == 0 and k == 0:
                    @pl.when(jnp.logical_not(own_out))
                    def _():
                        out_copy(s, k).wait_send()
                else:
                    out_copy(s, k).wait_send()

    for r in range(rows):
        pltpu.make_async_copy(fields_ref.at[0], out_ref.at[r], out_recv.at[r]).wait()


def body(n, fields, norm_gain, w_qkv, w_out):
    rows, cells, width = fields.shape
    hw = width // HEADS
    span = 2 * cells
    hbm = pl.BlockSpec(memory_space=pl.ANY)
    scratch = [
        pltpu.VMEM((rows, cells, width), BF16),
        pltpu.VMEM((1, width), F32),
        pltpu.VMEM((width, 3 * width), BF16),
        pltpu.VMEM((width, width), BF16),
        pltpu.VMEM((n, cells, width), BF16),
        pltpu.VMEM((2, cells, width), BF16),
        pltpu.VMEM((n * cells, 2 * width), BF16),
        pltpu.VMEM((2 * width, n * cells), BF16),
        pltpu.VMEM((4, 2 * width, span), BF16),
        pltpu.VMEM((2, 4 * cells, span), F32),
        pltpu.VMEM((2, 4 * cells, span), F32),
        pltpu.VMEM((2, 4 * cells, span), F32),
        pltpu.VMEM((2, 4 * cells, span), F32),
        pltpu.VMEM((4, HEADS, 1, span), F32),
        pltpu.VMEM((4, HEADS, 2 * hw, span), F32),
        pltpu.VMEM((4, 2, 2, 1, span), F32),
        pltpu.VMEM((4, width, span), BF16),
        pltpu.VMEM((4, span, width), BF16),
        pltpu.SemaphoreType.DMA((4,)),
        pltpu.SemaphoreType.DMA((n, 2)),
        pltpu.SemaphoreType.DMA((n, 2)),
        pltpu.SemaphoreType.DMA((n,)),
        pltpu.SemaphoreType.DMA((4, 2)),
        pltpu.SemaphoreType.DMA((rows,)),
        pltpu.SemaphoreType.REGULAR((1,)),
    ]
    return pl.pallas_call(
        functools.partial(kernel, n),
        out_shape=jax.ShapeDtypeStruct(fields.shape, fields.dtype),
        in_specs=[hbm] * 4,
        out_specs=hbm,
        scratch_shapes=scratch,
        compiler_params=pltpu.CompilerParams(collective_id=0, has_side_effects=True),
        name="axial",
    )(fields, norm_gain.reshape(1, width), w_qkv, w_out)


def solution(mesh):
    return jax.shard_map(
        functools.partial(body, mesh.shape["lon"]),
        mesh=mesh,
        in_specs=(P(("groups", "lat"), "lon", None), P(), P(), P()),
        out_specs=P(("groups", "lat"), "lon", None),
        check_vma=False,
    )
```

```python
import functools
import math

import jax
import jax.numpy as jnp
from jax import lax
from jax.experimental import pallas as pl
from jax.experimental.pallas import tpu as pltpu
from jax.sharding import PartitionSpec as P

HEADS = 8
LOG2E = math.log2(math.e)
LOW = -1e30
AHEAD = 2
PLAN = [[], [(1, 0)], [(2, 0)], [(2, 1), (3, 0), (3, 1), (1, 1), (0, 0), (0, 1)]]
F32 = jnp.float32
BF16 = jnp.bfloat16
MESH = pl.DeviceIdType.MESH


def kernel(
    n,
    fields_ref, gain_ref, wqkv_ref, wout_ref, out_ref,
    xin, gain, wqkv, wout, raw, nbuf, kd, vt, qt, sbuf0, sbuf1, sbuf2, sbuf3, mst, ost, alpha, att, obuf,
    load_sem, raw_send, raw_recv, fwd_send, out_send, out_recv, ready,
):
    rows, cells, width = xin.shape
    total_rows = 2 * rows
    half = cells // 2
    hw = width // HEADS
    span = 2 * cells
    tile = 2 * cells
    keys = 8 * cells
    sbufs = (sbuf0, sbuf1, sbuf2, sbuf3)

    p = lax.axis_index("lon")
    j = lax.axis_index("lat")
    right = {"lon": lax.rem(p + 1, n), "lat": j}
    left = {"lon": lax.rem(p + n - 1, n), "lat": j}
    partner = {"lon": p, "lat": 1 - j}

    loads = [
        pltpu.make_async_copy(fields_ref, xin, load_sem.at[0]),
        pltpu.make_async_copy(gain_ref, gain, load_sem.at[1]),
        pltpu.make_async_copy(wqkv_ref, wqkv, load_sem.at[2]),
        pltpu.make_async_copy(wout_ref, wout, load_sem.at[3]),
    ]
    for load in loads:
        load.start()

    barrier = pltpu.get_barrier_semaphore()
    for dist in range(n // 4, 0, -1):
        for step in {dist, n - dist}:
            for core in (0, 1):
                pl.semaphore_signal(
                    barrier, inc=1, device_id={"lon": lax.rem(p + step, n), "lat": core}, device_id_type=MESH
                )
    pl.semaphore_signal(barrier, inc=1, device_id=partner, device_id_type=MESH)

    def row_of(x):
        return (x * total_rows + n - 1) // n

    def takes_row(x):
        return (row_of(x) * n) // total_rows == x

    my_row = row_of(p)
    main = takes_row(p)
    my_lat = my_row // rows
    my_r = lax.rem(my_row, rows)

    def field_copy(d, h):
        x = lax.rem(p + n - d, n)
        r = lax.rem(row_of(x), rows)
        return pltpu.make_async_remote_copy(
            src_ref=xin.at[r, pl.ds(h * half, half)],
            dst_ref=raw.at[d, pl.ds(h * half, half)],
            send_sem=raw_send.at[d, h],
            recv_sem=raw_recv.at[d, h],
            device_id={"lon": x, "lat": h},
            device_id_type=MESH,
        )

    def own_field_copy(h):
        return pltpu.make_async_copy(
            fields_ref.at[my_r, pl.ds(h * half, half)], raw.at[0, pl.ds(h * half, half)], raw_recv.at[0, h]
        )

    def sends_to(d):
        x = lax.rem(p + n - d, n)
        return jnp.logical_and(takes_row(x), row_of(x) // rows == j)

    def start_fields(d):
        @pl.when(sends_to(d))
        def _():
            for h in (0, 1):
                if isinstance(d, int) and d == 0:
                    @pl.when(j == h)
                    def _():
                        own_field_copy(h).start()

                    @pl.when(j != h)
                    def _():
                        field_copy(d, h).start()
                else:
                    field_copy(d, h).start()

    def forward(d):
        return pltpu.make_async_remote_copy(
            src_ref=raw.at[d, pl.ds(j * half, half)],
            dst_ref=raw.at[d, pl.ds(j * half, half)],
            send_sem=fwd_send.at[d],
            recv_sem=raw_recv.at[d, j],
            device_id=partner,
            device_id_type=MESH,
        )

    def wait_half(d, h):
        pltpu.make_async_copy(
            fields_ref.at[0, pl.ds(0, half)], raw.at[d, pl.ds(h * half, half)], raw_recv.at[d, h]
        ).wait()

    def take(d):
        wait_half(d, j)
        forward(d).start()

    loads[0].wait()
    pl.semaphore_wait(barrier, n + 1)
    for side, step in enumerate((n // 4, n - n // 4)):
        pl.semaphore_signal(
            ready.at[side], inc=1, device_id={"lon": lax.rem(p + step, n), "lat": j}, device_id_type=MESH
        )
    start_fields(0)
    for dist in range(1, n // 4 + 1):
        start_fields(dist)
        start_fields(n - dist)
    low = (p + n - n // 4) // n
    pl.semaphore_wait(ready.at[1 - low], 1)
    for dist in range(n // 2, n // 4, -1):
        start_fields(low * dist + (1 - low) * (n - dist))
    pl.semaphore_wait(ready.at[low], 1)
    for dist in range(n // 2 - 1, n // 4, -1):
        start_fields(low * (n - dist) + (1 - low) * dist)

    for load in loads[1:]:
        load.wait()

    def stage_chunks(g):
        return (2 * g, 2 * g + 1), (n - 1 - 2 * g, n - 2 - 2 * g)

    def own_chunk(g, k):
        return 2 * g + k + j * (n - 1 - 4 * g - 2 * k)

    def order_of(s):
        return s + s // 2 - 2 * (s // 3)

    def out_copy(s, k):
        d = own_chunk(order_of(s), k)
        return pltpu.make_async_remote_copy(
            src_ref=obuf.at[s, pl.ds(k * cells, cells)],
            dst_ref=out_ref.at[my_r],
            send_sem=out_send.at[s, k],
            recv_sem=out_recv.at[my_r],
            device_id={"lon": lax.rem(p + d, n), "lat": my_lat},
            device_id_type=MESH,
        )

    own_out = jnp.logical_and(j == 0, my_lat == 0)

    def own_out_copy():
        return pltpu.make_async_copy(obuf.at[0, pl.ds(0, cells)], out_ref.at[my_r], out_recv.at[my_r])

    @pl.when(main)
    def _():
        wq = wqkv[:, :width]
        wk = wqkv[:, width : 2 * width]
        wv = wqkv[:, 2 * width :]
        for h in range(HEADS):
            vt[pl.ds(2 * hw * h + hw, hw), :] = jnp.ones((hw, n * cells), BF16)

        def clear(h, carry):
            for s in range(4):
                mst[s, h] = jnp.full(mst.shape[2:], LOW, F32)
                ost[s, h] = jnp.zeros(ost.shape[2:], F32)
            return carry

        lax.fori_loop(0, HEADS, clear, 0)

        def project(slot, d, place):
            x = raw[d].astype(F32)
            center = jnp.mean(x, axis=-1, keepdims=True)
            y = x - center
            spread = jnp.mean(y * y, axis=-1, keepdims=True)
            normed = (y * lax.rsqrt(spread + 1e-05) * gain[...]).astype(BF16)
            nbuf[place] = normed
            where = pl.ds(slot * cells, cells)
            k = jnp.dot(normed, wk, preferred_element_type=F32).astype(BF16)
            kd[where, :width] = k
            kd[where, width:] = k
            v = lax.dot_general(wv, normed, (((0,), (1,)), ((), ())), preferred_element_type=F32).astype(BF16)
            for h in range(HEADS):
                vt[2 * hw * h : 2 * hw * h + hw, where] = v[hw * h : hw * h + hw]

        def takes(s):
            sides = stage_chunks(order_of(s))
            for k in (0, 1):
                for side in sides:
                    take(side[k])

        def arrive(s):
            sides = stage_chunks(order_of(s))
            for k in (0, 1):
                for place in (0, 1):
                    d = sides[place][k]
                    wait_half(d, 1 - j)
                    project(4 * s + 2 * place + k, d, place)
                q = lax.dot_general(wq, nbuf[j], (((0,), (1,)), ((), ())), preferred_element_type=F32)
                q = (q * (1.0 / math.sqrt(hw))).astype(BF16).astype(F32) * LOG2E
                high = q.astype(BF16)
                low = (q - high.astype(F32)).astype(BF16)
                where = pl.ds(k * cells, cells)
                qt[s, :width, where] = high
                qt[s, width:, where] = low

        def score_steps(unit, slot):
            heads, qb, kg = unit
            high = {}

            def queries(h):
                gap = jnp.zeros((hw, span), BF16)
                return jnp.concatenate(
                    [
                        qt[qb, pl.ds(base + hw * other, hw), :] if other == h else gap
                        for base in (0, width)
                        for other in range(HEADS)
                    ],
                    axis=0,
                )

            of = [queries(h) for h in heads]

            def step(t):
                for i, q in enumerate(of):
                    where = pl.ds(pl.multiple_of(kg * keys, keys) + t * tile, tile)
                    s = jnp.dot(kd[where, :], q, preferred_element_type=F32)
                    sbufs[slot][i, pl.ds(t * tile, tile), :] = s
                    peak = jnp.max(s.reshape(tile // 8, 8, span), axis=0)
                    high[i] = peak if t == 0 else jnp.maximum(high[i], peak)

            def end():
                for i, h in enumerate(heads):
                    old = mst[qb, h]
                    new = jnp.maximum(old, jnp.max(high[i], axis=0, keepdims=True))
                    mst[qb, h] = new
                    alpha[slot, i, 0] = new
                    alpha[slot, i, 1] = jnp.exp2(old - new)

            return step, end

        def value_steps(unit, slot):
            heads, qb, kg = unit
            total = {i: ost[qb, h] * alpha[slot, i, 1] for i, h in enumerate(heads)}

            def step(t):
                for i, h in enumerate(heads):
                    e = jnp.exp2(sbufs[slot][i, pl.ds(t * tile, tile), :] - alpha[slot, i, 0]).astype(BF16)
                    where = pl.ds(pl.multiple_of(kg * keys, keys) + t * tile, tile)
                    v = vt[pl.ds(2 * hw * h, 2 * hw), where]
                    total[i] = total[i] + jnp.dot(v, e, preferred_element_type=F32)

            def end():
                for i, h in enumerate(heads):
                    ost[qb, h] = total[i]
                    att[qb, pl.ds(h * hw, hw), :] = (total[i][:hw] / total[i][hw:]).astype(BF16)

            return step, end

        def both(score_of, value_of):
            a = None if score_of is None else score_steps(*score_of)
            b = None if value_of is None else value_steps(*value_of)
            for t in range(keys // tile):
                if a:
                    a[0](t)
                if b:
                    b[0](t)
            if a:
                a[1]()
            if b:
                b[1]()

        units = HEADS // 2

        def run(combo, count, final):
            def unit(i, a):
                qb, kg = combo(i + a // units)
                a = a % units
                return ((2 * a, 2 * a + 1), qb, kg), a

            for a in range(AHEAD):
                both(unit(0, a), None)

            def step(i, carry):
                for a in range(units):
                    both(unit(i, a + AHEAD), unit(i, a))
                if final:
                    qb, kg = combo(i)

                    @pl.when(kg == 1)
                    def _():
                        finish(qb)

                return carry

            if count > 1:
                lax.fori_loop(0, count - 1, step, 0)
            for a in range(units):
                both(unit(count - 1, a + AHEAD) if a + AHEAD < units else None, unit(count - 1, a))
            if final:
                finish(combo(count - 1)[0])

        def finish(s):
            result = lax.dot_general(
                att[s], wout[...], (((0,), (0,)), ((), ())), preferred_element_type=F32
            )
            group = order_of(s)
            for k in (1, 0):
                here = pl.ds(k * cells, cells)
                d = own_chunk(group, k)
                obuf[s, here, :] = (result[k * cells : (k + 1) * cells] + raw[d].astype(F32)).astype(BF16)
                if k == 0:
                    own = jnp.logical_and(own_out, s == 0)

                    @pl.when(own)
                    def _():
                        own_out_copy().start()

                    @pl.when(jnp.logical_not(own))
                    def _():
                        out_copy(s, k).start()
                else:
                    out_copy(s, k).start()

        def pick(values, i):
            count = len(values)
            got = values[0]
            for k in range(1, count):
                if values[k] != values[k - 1]:
                    got = got + (values[k] - values[k - 1]) * ((i + count - k) // count)
            return got

        takes(0)
        takes(1)
        for s, combos in enumerate(PLAN):
            arrive(s)
            if s in (1, 2):
                takes(s + 1)
            if combos:
                blocks, groups = zip(*combos)
                run(lambda i, b=blocks, g=groups: (pick(b, i), pick(g, i)), len(combos), s == 3)

    for d in range(n):
        @pl.when(sends_to(d))
        def _():
            for h in (0, 1):
                if d == 0:
                    @pl.when(j != h)
                    def _():
                        field_copy(d, h).wait_send()
                else:
                    field_copy(d, h).wait_send()

    @pl.when(main)
    def _():
        for d in range(n):
            forward(d).wait_send()
        for s in range(4):
            for k in (0, 1):
                if s == 0 and k == 0:
                    @pl.when(jnp.logical_not(own_out))
                    def _():
                        out_copy(s, k).wait_send()
                else:
                    out_copy(s, k).wait_send()

    for r in range(rows):
        pltpu.make_async_copy(fields_ref.at[0], out_ref.at[r], out_recv.at[r]).wait()


def body(n, fields, norm_gain, w_qkv, w_out):
    rows, cells, width = fields.shape
    hw = width // HEADS
    span = 2 * cells
    hbm = pl.BlockSpec(memory_space=pl.ANY)
    scratch = [
        pltpu.VMEM((rows, cells, width), BF16),
        pltpu.VMEM((1, width), F32),
        pltpu.VMEM((width, 3 * width), BF16),
        pltpu.VMEM((width, width), BF16),
        pltpu.VMEM((n, cells, width), BF16),
        pltpu.VMEM((2, cells, width), BF16),
        pltpu.VMEM((n * cells, 2 * width), BF16),
        pltpu.VMEM((2 * width, n * cells), BF16),
        pltpu.VMEM((4, 2 * width, span), BF16),
        pltpu.VMEM((2, 8 * cells, span), F32),
        pltpu.VMEM((2, 8 * cells, span), F32),
        pltpu.VMEM((2, 8 * cells, span), F32),
        pltpu.VMEM((2, 8 * cells, span), F32),
        pltpu.VMEM((4, HEADS, 1, span), F32),
        pltpu.VMEM((4, HEADS, 2 * hw, span), F32),
        pltpu.VMEM((4, 2, 2, 1, span), F32),
        pltpu.VMEM((4, width, span), BF16),
        pltpu.VMEM((4, span, width), BF16),
        pltpu.SemaphoreType.DMA((4,)),
        pltpu.SemaphoreType.DMA((n, 2)),
        pltpu.SemaphoreType.DMA((n, 2)),
        pltpu.SemaphoreType.DMA((n,)),
        pltpu.SemaphoreType.DMA((4, 2)),
        pltpu.SemaphoreType.DMA((rows,)),
        pltpu.SemaphoreType.REGULAR((2,)),
    ]
    return pl.pallas_call(
        functools.partial(kernel, n),
        out_shape=jax.ShapeDtypeStruct(fields.shape, fields.dtype),
        in_specs=[hbm] * 4,
        out_specs=hbm,
        scratch_shapes=scratch,
        compiler_params=pltpu.CompilerParams(collective_id=0, has_side_effects=True),
        name="axial",
    )(fields, norm_gain.reshape(1, width), w_qkv, w_out)


def solution(mesh):
    return jax.shard_map(
        functools.partial(body, mesh.shape["lon"]),
        mesh=mesh,
        in_specs=(P(("groups", "lat"), "lon", None), P(), P(), P()),
        out_specs=P(("groups", "lat"), "lon", None),
        check_vma=False,
    )
```

```python
import functools
import math

import jax
import jax.numpy as jnp
from jax import lax
from jax.experimental import pallas as pl
from jax.experimental.pallas import tpu as pltpu
from jax.sharding import PartitionSpec as P

HEADS = 8
LOG2E = math.log2(math.e)
LOW = -1e30
AHEAD = 2
PLAN = [[], [(1, 0)], [(2, 0)], [(2, 1), (1, 1), (3, 0), (3, 1), (0, 0), (0, 1)]]
F32 = jnp.float32
BF16 = jnp.bfloat16
MESH = pl.DeviceIdType.MESH


def kernel(
    n,
    fields_ref, gain_ref, wqkv_ref, wout_ref, out_ref,
    xin, gain, wqkv, wout, raw, nbuf, kd, vt, qt, sbuf0, sbuf1, sbuf2, sbuf3, mst, ost, alpha, att, obuf,
    load_sem, raw_send, raw_recv, fwd_send, out_send, out_recv, ready,
):
    rows, cells, width = xin.shape
    total_rows = 2 * rows
    half = cells // 2
    hw = width // HEADS
    span = 2 * cells
    tile = 2 * cells
    keys = 8 * cells
    sbufs = (sbuf0, sbuf1, sbuf2, sbuf3)

    p = lax.axis_index("lon")
    j = lax.axis_index("lat")
    right = {"lon": lax.rem(p + 1, n), "lat": j}
    left = {"lon": lax.rem(p + n - 1, n), "lat": j}
    partner = {"lon": p, "lat": 1 - j}

    loads = [
        pltpu.make_async_copy(fields_ref, xin, load_sem.at[0]),
        pltpu.make_async_copy(gain_ref, gain, load_sem.at[1]),
        pltpu.make_async_copy(wqkv_ref, wqkv, load_sem.at[2]),
        pltpu.make_async_copy(wout_ref, wout, load_sem.at[3]),
    ]
    for load in loads:
        load.start()

    barrier = pltpu.get_barrier_semaphore()
    for dist in range(n // 4, 0, -1):
        for step in {dist, n - dist}:
            for core in (0, 1):
                pl.semaphore_signal(
                    barrier, inc=1, device_id={"lon": lax.rem(p + step, n), "lat": core}, device_id_type=MESH
                )
    pl.semaphore_signal(barrier, inc=1, device_id=partner, device_id_type=MESH)

    def row_of(x):
        return (x * total_rows + n - 1) // n

    def takes_row(x):
        return (row_of(x) * n) // total_rows == x

    my_row = row_of(p)
    main = takes_row(p)
    my_lat = my_row // rows
    my_r = lax.rem(my_row, rows)

    def field_copy(d, h):
        x = lax.rem(p + n - d, n)
        r = lax.rem(row_of(x), rows)
        return pltpu.make_async_remote_copy(
            src_ref=xin.at[r, pl.ds(h * half, half)],
            dst_ref=raw.at[d, pl.ds(h * half, half)],
            send_sem=raw_send.at[d, h],
            recv_sem=raw_recv.at[d, h],
            device_id={"lon": x, "lat": h},
            device_id_type=MESH,
        )

    def own_field_copy(h):
        return pltpu.make_async_copy(
            fields_ref.at[my_r, pl.ds(h * half, half)], raw.at[0, pl.ds(h * half, half)], raw_recv.at[0, h]
        )

    def sends_to(d):
        x = lax.rem(p + n - d, n)
        return jnp.logical_and(takes_row(x), row_of(x) // rows == j)

    def start_fields(d):
        @pl.when(sends_to(d))
        def _():
            for h in (0, 1):
                if isinstance(d, int) and d == 0:
                    @pl.when(j == h)
                    def _():
                        own_field_copy(h).start()

                    @pl.when(j != h)
                    def _():
                        field_copy(d, h).start()
                else:
                    field_copy(d, h).start()

    def forward(d):
        return pltpu.make_async_remote_copy(
            src_ref=raw.at[d, pl.ds(j * half, half)],
            dst_ref=raw.at[d, pl.ds(j * half, half)],
            send_sem=fwd_send.at[d],
            recv_sem=raw_recv.at[d, j],
            device_id=partner,
            device_id_type=MESH,
        )

    def wait_half(d, h):
        pltpu.make_async_copy(
            fields_ref.at[0, pl.ds(0, half)], raw.at[d, pl.ds(h * half, half)], raw_recv.at[d, h]
        ).wait()

    def take(d):
        wait_half(d, j)
        forward(d).start()

    loads[0].wait()
    pl.semaphore_wait(barrier, n + 1)
    for side, step in enumerate((n // 4, n - n // 4)):
        pl.semaphore_signal(
            ready.at[side], inc=1, device_id={"lon": lax.rem(p + step, n), "lat": j}, device_id_type=MESH
        )
    start_fields(0)
    for dist in range(1, n // 4 + 1):
        start_fields(dist)
        start_fields(n - dist)
    low = (p + n - n // 4) // n
    pl.semaphore_wait(ready.at[1 - low], 1)
    for dist in range(n // 2, n // 4, -1):
        start_fields(low * dist + (1 - low) * (n - dist))
    pl.semaphore_wait(ready.at[low], 1)
    for dist in range(n // 2 - 1, n // 4, -1):
        start_fields(low * (n - dist) + (1 - low) * dist)

    for load in loads[1:]:
        load.wait()

    def stage_chunks(g):
        return (2 * g, 2 * g + 1), (n - 1 - 2 * g, n - 2 - 2 * g)

    def own_chunk(g, k):
        return 2 * g + k + j * (n - 1 - 4 * g - 2 * k)

    def order_of(s):
        return s + s // 2 - 2 * (s // 3)

    def out_copy(s, k):
        d = own_chunk(order_of(s), k)
        return pltpu.make_async_remote_copy(
            src_ref=obuf.at[s, pl.ds(k * cells, cells)],
            dst_ref=out_ref.at[my_r],
            send_sem=out_send.at[s, k],
            recv_sem=out_recv.at[my_r],
            device_id={"lon": lax.rem(p + d, n), "lat": my_lat},
            device_id_type=MESH,
        )

    own_out = jnp.logical_and(j == 0, my_lat == 0)

    def own_out_copy():
        return pltpu.make_async_copy(obuf.at[0, pl.ds(0, cells)], out_ref.at[my_r], out_recv.at[my_r])

    @pl.when(main)
    def _():
        wq = wqkv[:, :width]
        wk = wqkv[:, width : 2 * width]
        wv = wqkv[:, 2 * width :]
        for h in range(HEADS):
            vt[pl.ds(2 * hw * h + hw, hw), :] = jnp.ones((hw, n * cells), BF16)

        def clear(h, carry):
            for s in range(4):
                mst[s, h] = jnp.full(mst.shape[2:], LOW, F32)
                ost[s, h] = jnp.zeros(ost.shape[2:], F32)
            return carry

        lax.fori_loop(0, HEADS, clear, 0)

        def project(slot, d, place):
            x = raw[d].astype(F32)
            center = jnp.mean(x, axis=-1, keepdims=True)
            y = x - center
            spread = jnp.mean(y * y, axis=-1, keepdims=True)
            normed = (y * lax.rsqrt(spread + 1e-05) * gain[...]).astype(BF16)
            nbuf[place] = normed
            where = pl.ds(slot * cells, cells)
            k = jnp.dot(normed, wk, preferred_element_type=F32).astype(BF16)
            kd[where, :width] = k
            kd[where, width:] = k
            v = lax.dot_general(wv, normed, (((0,), (1,)), ((), ())), preferred_element_type=F32).astype(BF16)
            for h in range(HEADS):
                vt[2 * hw * h : 2 * hw * h + hw, where] = v[hw * h : hw * h + hw]

        def takes(s):
            sides = stage_chunks(order_of(s))
            for k in (0, 1):
                for side in sides:
                    take(side[k])

        def arrive(s):
            sides = stage_chunks(order_of(s))
            for k in (0, 1):
                for place in (0, 1):
                    d = sides[place][k]
                    wait_half(d, 1 - j)
                    project(4 * s + 2 * place + k, d, place)
                q = lax.dot_general(wq, nbuf[j], (((0,), (1,)), ((), ())), preferred_element_type=F32)
                q = (q * (1.0 / math.sqrt(hw))).astype(BF16).astype(F32) * LOG2E
                high = q.astype(BF16)
                low = (q - high.astype(F32)).astype(BF16)
                where = pl.ds(k * cells, cells)
                qt[s, :width, where] = high
                qt[s, width:, where] = low

        def score_steps(unit, slot):
            heads, qb, kg = unit
            high = {}

            def queries(h):
                gap = jnp.zeros((hw, span), BF16)
                return jnp.concatenate(
                    [
                        qt[qb, pl.ds(base + hw * other, hw), :] if other == h else gap
                        for base in (0, width)
                        for other in range(HEADS)
                    ],
                    axis=0,
                )

            of = [queries(h) for h in heads]

            def step(t):
                for i, q in enumerate(of):
                    where = pl.ds(pl.multiple_of(kg * keys, keys) + t * tile, tile)
                    s = jnp.dot(kd[where, :], q, preferred_element_type=F32)
                    sbufs[slot][i, pl.ds(t * tile, tile), :] = s
                    peak = jnp.max(s.reshape(tile // 8, 8, span), axis=0)
                    high[i] = peak if t == 0 else jnp.maximum(high[i], peak)

            def end():
                for i, h in enumerate(heads):
                    old = mst[qb, h]
                    new = jnp.maximum(old, jnp.max(high[i], axis=0, keepdims=True))
                    mst[qb, h] = new
                    alpha[slot, i, 0] = new
                    alpha[slot, i, 1] = jnp.exp2(old - new)

            return step, end

        def value_steps(unit, slot):
            heads, qb, kg = unit
            total = {i: ost[qb, h] * alpha[slot, i, 1] for i, h in enumerate(heads)}

            def step(t):
                for i, h in enumerate(heads):
                    e = jnp.exp2(sbufs[slot][i, pl.ds(t * tile, tile), :] - alpha[slot, i, 0]).astype(BF16)
                    where = pl.ds(pl.multiple_of(kg * keys, keys) + t * tile, tile)
                    v = vt[pl.ds(2 * hw * h, 2 * hw), where]
                    total[i] = total[i] + jnp.dot(v, e, preferred_element_type=F32)

            def end():
                for i, h in enumerate(heads):
                    ost[qb, h] = total[i]
                    att[qb, pl.ds(h * hw, hw), :] = (total[i][:hw] / total[i][hw:]).astype(BF16)

            return step, end

        def both(score_of, value_of):
            a = None if score_of is None else score_steps(*score_of)
            b = None if value_of is None else value_steps(*value_of)
            for t in range(keys // tile):
                if a:
                    a[0](t)
                if b:
                    b[0](t)
            if a:
                a[1]()
            if b:
                b[1]()

        units = HEADS // 2

        def run(combo, count, final):
            def unit(i, a):
                qb, kg = combo(i + a // units)
                a = a % units
                return ((2 * a, 2 * a + 1), qb, kg), a

            for a in range(AHEAD):
                both(unit(0, a), None)

            def step(i, carry):
                for a in range(units):
                    both(unit(i, a + AHEAD), unit(i, a))
                if final:
                    qb, kg = combo(i)

                    @pl.when(kg == 1)
                    def _():
                        finish(qb)

                return carry

            if count > 1:
                lax.fori_loop(0, count - 1, step, 0)
            for a in range(units):
                both(unit(count - 1, a + AHEAD) if a + AHEAD < units else None, unit(count - 1, a))
            if final:
                finish(combo(count - 1)[0])

        def finish(s):
            result = lax.dot_general(
                att[s], wout[...], (((0,), (0,)), ((), ())), preferred_element_type=F32
            )
            group = order_of(s)
            for k in (1, 0):
                here = pl.ds(k * cells, cells)
                d = own_chunk(group, k)
                obuf[s, here, :] = (result[k * cells : (k + 1) * cells] + raw[d].astype(F32)).astype(BF16)
                if k == 0:
                    own = jnp.logical_and(own_out, s == 0)

                    @pl.when(own)
                    def _():
                        own_out_copy().start()

                    @pl.when(jnp.logical_not(own))
                    def _():
                        out_copy(s, k).start()
                else:
                    out_copy(s, k).start()

        def pick(values, i):
            count = len(values)
            got = values[0]
            for k in range(1, count):
                if values[k] != values[k - 1]:
                    got = got + (values[k] - values[k - 1]) * ((i + count - k) // count)
            return got

        takes(0)
        takes(1)
        for s, combos in enumerate(PLAN):
            arrive(s)
            if s in (1, 2):
                takes(s + 1)
            if combos:
                blocks, groups = zip(*combos)
                run(lambda i, b=blocks, g=groups: (pick(b, i), pick(g, i)), len(combos), s == 3)

    for d in range(n):
        @pl.when(sends_to(d))
        def _():
            for h in (0, 1):
                if d == 0:
                    @pl.when(j != h)
                    def _():
                        field_copy(d, h).wait_send()
                else:
                    field_copy(d, h).wait_send()

    @pl.when(main)
    def _():
        for d in range(n):
            forward(d).wait_send()
        for s in range(4):
            for k in (0, 1):
                if s == 0 and k == 0:
                    @pl.when(jnp.logical_not(own_out))
                    def _():
                        out_copy(s, k).wait_send()
                else:
                    out_copy(s, k).wait_send()

    for r in range(rows):
        pltpu.make_async_copy(fields_ref.at[0], out_ref.at[r], out_recv.at[r]).wait()


def body(n, fields, norm_gain, w_qkv, w_out):
    rows, cells, width = fields.shape
    hw = width // HEADS
    span = 2 * cells
    hbm = pl.BlockSpec(memory_space=pl.ANY)
    scratch = [
        pltpu.VMEM((rows, cells, width), BF16),
        pltpu.VMEM((1, width), F32),
        pltpu.VMEM((width, 3 * width), BF16),
        pltpu.VMEM((width, width), BF16),
        pltpu.VMEM((n, cells, width), BF16),
        pltpu.VMEM((2, cells, width), BF16),
        pltpu.VMEM((n * cells, 2 * width), BF16),
        pltpu.VMEM((2 * width, n * cells), BF16),
        pltpu.VMEM((4, 2 * width, span), BF16),
        pltpu.VMEM((2, 8 * cells, span), F32),
        pltpu.VMEM((2, 8 * cells, span), F32),
        pltpu.VMEM((2, 8 * cells, span), F32),
        pltpu.VMEM((2, 8 * cells, span), F32),
        pltpu.VMEM((4, HEADS, 1, span), F32),
        pltpu.VMEM((4, HEADS, 2 * hw, span), F32),
        pltpu.VMEM((4, 2, 2, 1, span), F32),
        pltpu.VMEM((4, width, span), BF16),
        pltpu.VMEM((4, span, width), BF16),
        pltpu.SemaphoreType.DMA((4,)),
        pltpu.SemaphoreType.DMA((n, 2)),
        pltpu.SemaphoreType.DMA((n, 2)),
        pltpu.SemaphoreType.DMA((n,)),
        pltpu.SemaphoreType.DMA((4, 2)),
        pltpu.SemaphoreType.DMA((rows,)),
        pltpu.SemaphoreType.REGULAR((2,)),
    ]
    return pl.pallas_call(
        functools.partial(kernel, n),
        out_shape=jax.ShapeDtypeStruct(fields.shape, fields.dtype),
        in_specs=[hbm] * 4,
        out_specs=hbm,
        scratch_shapes=scratch,
        compiler_params=pltpu.CompilerParams(collective_id=0, has_side_effects=True),
        name="axial",
    )(fields, norm_gain.reshape(1, width), w_qkv, w_out)


def solution(mesh):
    return jax.shard_map(
        functools.partial(body, mesh.shape["lon"]),
        mesh=mesh,
        in_specs=(P(("groups", "lat"), "lon", None), P(), P(), P()),
        out_specs=P(("groups", "lat"), "lon", None),
        check_vma=False,
    )
```
